128 devices in a mesh: row: 16 (over y, z), col: 8 (over x, core).
Axes of the slice: x: 4, y: 4, z: 4, core: 2. Of those that a mesh axis runs over, the one named last changes fastest.
Arguments:
- matrix: bfloat16 [3, 8192, 6, 4096], P(None, 'row', None, 'col'), may hold values from -6 to 6
- multiplier: bfloat16 [2, 512, 512], replicated
- checksum_weight: float32 [3, 8192], P(None, 'row')
Outputs:
- factored: bfloat16 [3, 8192, 6, 4096], P(None, 'row', None, 'col')
- group_checksum: float32 [16, 6, 4096], P('row', None, 'col')
- total_checksum: float32 [6, 4096], P(None, 'col')
The draws below stay inside these ranges and needn't reach their ends.
All inputs are finite; a program needn't handle non-finite values.
Results may differ from the reference program's by a relative error of at most 0.0056.
Values may be sent and summed in bfloat16 or wider, within the bound.
No kernel may reach another device: no remote copies, remote signals or barrier semaphores. Data moves between devices by JAX's collectives and lax.ppermute only.
A program may use at most 192 MiB of HBM per device.

```python
import math
import jax
import jax.numpy as jnp
from jax import lax

PANEL_WIDTH = 512
ORDER = 24576
ELIMINATION_STEPS = 2
RBD = 3
CBD = 6
N_ROW = 16
N_COL = 8


def draw_multiplier(key, part):
    first_key, second_key = jax.random.split(jax.random.fold_in(key, 11))
    base = 2.0 * math.sqrt(PANEL_WIDTH)
    diagonal = jnp.exp(jax.random.uniform(first_key, (ELIMINATION_STEPS, PANEL_WIDTH), jnp.float32, math.log(0.5), math.log(2.0))) / base
    offdiag = jax.random.normal(second_key, (ELIMINATION_STEPS, PANEL_WIDTH, PANEL_WIDTH), jnp.float32) * (0.3 / (base * math.sqrt(PANEL_WIDTH)))
    identity = jnp.eye(PANEL_WIDTH, dtype=jnp.float32)
    return (offdiag + identity[None, :, :] * diagonal[:, :, None]).astype(jnp.bfloat16)


def draw_checksum_weight(key, part):
    sub_key = jax.random.fold_in(key, 23)
    group = (jnp.arange(N_ROW * PANEL_WIDTH, dtype=jnp.int32) // PANEL_WIDTH).astype(jnp.float32)
    rising = 1.0 + 2.0 * group / max(N_ROW - 1, 1)
    scale = 0.5 / math.sqrt(RBD * PANEL_WIDTH)
    values = jax.random.normal(sub_key, (RBD, N_ROW * PANEL_WIDTH), jnp.float32)
    return (values * rising[None, :] * scale).astype(jnp.float32)


def level_of(key, shape, shards, least, high):
    factor_of, own = 1.0, jax.random.fold_in(key, 6)
    for dim, parts in shards:
        draws = jnp.exp(jax.random.uniform(jax.random.fold_in(own, dim), (parts,), jnp.float32, least / len(shards), high / len(shards)))
        factor_of = factor_of * jnp.repeat(draws, shape[dim] // parts).reshape([-1 if axis == dim else 1 for axis in range(len(shape))])
    return factor_of


def gaussian(key, shape, spread, reach, shards=(), kind=jnp.bfloat16):
    values = jax.random.normal(key, shape, jnp.float32) * spread
    if len(shards) > 0:
        values = level_of(key, shape, shards, -0.22, 0.18) * values
    return jnp.clip(values, min=-reach, max=reach).astype(kind)


def setup_inputs(seed: int = 0) -> dict:
    splits = jax.random.split(jax.random.key(seed), 4)
    return {
        "matrix": gaussian(splits[0], (RBD, N_ROW * PANEL_WIDTH, CBD, N_COL * PANEL_WIDTH), 1.0, 6.0, ((1, 16), (3, 8))),
        "multiplier": draw_multiplier(jax.random.fold_in(splits[3], 71), 0),
        "checksum_weight": draw_checksum_weight(jax.random.fold_in(splits[3], 71), 0),
    }


slab_rows = 4096


def reference(matrix, multiplier, checksum_weight):
    highest_precision = lax.Precision.HIGHEST
    full_matrix_input = matrix.reshape(ORDER, ORDER)
    weight_rows = checksum_weight.reshape(ORDER)
    group_of_row = (jnp.arange(ORDER, dtype=jnp.int32) // PANEL_WIDTH) % N_ROW
    selector = (group_of_row[None, :] == jnp.arange(N_ROW, dtype=jnp.int32)[:, None]).astype(jnp.float32) * weight_rows[None, :]
    checks = jnp.dot(selector, full_matrix_input.astype(jnp.float32), precision=highest_precision, preferred_element_type=jnp.float32)
    column_ids = jnp.arange(ORDER, dtype=jnp.int32)
    for eliminate_block in range(ELIMINATION_STEPS):
        column_begin = eliminate_block * PANEL_WIDTH
        column_end = column_begin + PANEL_WIDTH
        lower_triangle = jnp.dot(full_matrix_input[column_end:, column_begin:column_end].astype(jnp.float32), multiplier[eliminate_block].astype(jnp.float32), precision=highest_precision, preferred_element_type=jnp.float32).astype(jnp.bfloat16)
        pivot_row_band = jnp.where(column_ids[None, :] >= column_end, full_matrix_input[column_begin:column_end, :].astype(jnp.float32), jnp.float32(0.0))
        summed = jnp.dot(selector[:, column_end:], lower_triangle.astype(jnp.float32), precision=highest_precision, preferred_element_type=jnp.float32)
        checks = checks - jnp.dot(summed, pivot_row_band, precision=highest_precision, preferred_element_type=jnp.float32)
        lower_f = lower_triangle.astype(jnp.float32)
        pieces = [full_matrix_input[:column_end]]
        for slab_start in range(column_end, ORDER, slab_rows):
            slab_stop = min(slab_start + slab_rows, ORDER)
            product = jnp.dot(lower_f[slab_start - column_end:slab_stop - column_end], pivot_row_band, precision=highest_precision, preferred_element_type=jnp.float32)
            pieces.append((full_matrix_input[slab_start:slab_stop].astype(jnp.float32) - product).astype(jnp.bfloat16))
        full_matrix_input = jnp.concatenate(pieces, axis=0)
        full_matrix_input = full_matrix_input.at[column_end:, column_begin:column_end].set(lower_triangle)
    factored = full_matrix_input.reshape(RBD, N_ROW * PANEL_WIDTH, CBD, N_COL * PANEL_WIDTH)
    return factored, checks.reshape(N_ROW, CBD, N_COL * PANEL_WIDTH), jnp.sum(checks, axis=0).reshape(CBD, N_COL * PANEL_WIDTH)
```

```python
import functools

import jax
import jax.numpy as jnp
from jax import lax
from jax.experimental import pallas as pl
from jax.experimental.pallas import tpu as pltpu
from jax.sharding import Mesh
from jax.sharding import PartitionSpec as P

ROW = ("row_0", "row_1")
F32, BF16 = jnp.float32, jnp.bfloat16


def spread(pieces, axis, size, place):
    ahead = jnp.where(place == 1, jnp.roll(pieces, -1, axis=0), pieces)
    got = [ahead[0]]
    for shift in range(1, size):
        got.append(lax.ppermute(ahead[shift], axis, [(0, shift), (1, (1 + shift) % size)]))
    return lax.select_n(place, *got), lax.select_n((place + size - 1) % size, *got)


def gather(piece, axis, size, place):
    got = [piece]
    for shift in range(1, size):
        got.append(lax.ppermute(piece, axis, [(i, (i + shift) % size) for i in range(size)]))
    back = got[::-1]
    return lax.dynamic_slice_in_dim(jnp.stack(back + back[:-1]), size - 1 - place, size, 0)


def in_three(rows):
    high = rows.astype(BF16).astype(F32)
    middle = (rows - high).astype(BF16).astype(F32)
    low = rows - high - middle
    return jnp.concatenate([high, middle, low, jnp.zeros_like(rows)], axis=0).astype(BF16)


def times_rows(rows, right):
    product = jnp.dot(in_three(rows), right, preferred_element_type=F32)
    return product[0:8] + product[8:16] + product[16:24]


def weigh_kernel(weight_ref, tile_ref, out_ref):
    block_rows, _, width, _ = tile_ref.shape
    tile = tile_ref[...].reshape(block_rows * width, width)
    out_ref[0] = times_rows(weight_ref[...], tile)


def left_kernel(info_ref, panel_ref, corner_ref, multiplier_ref, weight_ref, left0_ref, left1_ref, sum_ref):
    step = pl.program_id(0)
    share = panel_ref.shape[2]
    width = corner_ref.shape[0]
    row = step * share + lax.broadcasted_iota(jnp.int32, (share, width), 0)
    my_row = info_ref[1]

    def keep(value, pivot):
        return jnp.where((row < width) & (my_row <= pivot), jnp.zeros_like(value), value)

    left0 = jnp.dot(panel_ref[0, 0], multiplier_ref[0], preferred_element_type=F32)
    left0 = keep(left0, 0).astype(BF16)
    column = jnp.dot(left0, corner_ref[...], preferred_element_type=F32)
    column = (panel_ref[0, 1].astype(F32) - column).astype(BF16)
    left1 = jnp.dot(column, multiplier_ref[1], preferred_element_type=F32)
    left1 = keep(left1, 1).astype(BF16)
    left0_ref[0] = left0
    left1_ref[0] = left1

    @pl.when(step == 0)
    def _():
        sum_ref[...] = jnp.zeros_like(sum_ref)

    sum_ref[0] += times_rows(weight_ref[0], left0)
    sum_ref[1] += times_rows(weight_ref[0], left1)


def trail_kernel(
    info_ref, left0_ref, left1_ref, second_ref, sums_ref, upper_ref, band_ref, base_ref, tile_ref, out_ref, check_ref
):
    width = second_ref.shape[0]
    first = pl.program_id(0) == 0
    my_col, my_row = info_ref[0], info_ref[1]
    upper0 = upper_ref[...].reshape(width, width)
    upper0 = jnp.where(first & (my_col == 0), jnp.zeros_like(upper0), upper0)
    upper1 = band_ref[...].reshape(width, width).astype(F32)
    upper1 = (upper1 - jnp.dot(second_ref[...], upper0, preferred_element_type=F32)).astype(BF16)
    upper1 = jnp.where(first & (my_col < 2), jnp.zeros_like(upper1), upper1)
    check_ref[0] = base_ref[0] - times_rows(sums_ref[0], upper0) - times_rows(sums_ref[1], upper1)
    for a in range(tile_ref.shape[0]):
        rows = slice(a * width, (a + 1) * width)
        product = jnp.dot(left0_ref[rows, :], upper0, preferred_element_type=F32)
        tile = (tile_ref[a, 0].astype(F32) - product).astype(BF16)
        product = jnp.dot(left1_ref[rows, :], upper1, preferred_element_type=F32)
        out_ref[a, 0] = (tile.astype(F32) - product).astype(BF16)
        for pivot, left_ref in enumerate((left0_ref, left1_ref)):
            below = True if a > 0 else my_row > pivot

            @pl.when(first & (my_col == pivot) & below)
            def _():
                out_ref[a, 0] = left_ref[rows, :]


def local(matrix, multiplier, checksum_weight):
    block_rows, block, cols, _ = matrix.shape
    grid_rows, grid_cols = lax.axis_size(ROW), lax.axis_size("col")
    my_row, my_col = lax.axis_index(ROW), lax.axis_index("col")
    info = jnp.stack([my_col, my_row]).astype(jnp.int32)
    tiles = matrix.transpose(0, 2, 1, 3)
    rows, piece, share = block_rows * block, block // grid_rows, block_rows * block // grid_cols
    weights = jnp.pad(checksum_weight.reshape(1, rows), ((0, 7), (0, 0)))
    smem = pl.BlockSpec(memory_space=pltpu.SMEM)
    column_of_tiles = pl.BlockSpec((block_rows, 1, block, block), lambda c: (0, c, 0, 0))
    one_check = pl.BlockSpec((1, 8, block), lambda c: (c, 0, 0))

    bands = tiles[0].reshape(cols, grid_rows, piece, block).transpose(1, 0, 2, 3)
    first, second = spread(bands, ROW, grid_rows, my_row)
    both = jnp.concatenate([first, second], axis=0)
    upper = lax.all_gather(both, ROW)

    both, panel = lax.optimization_barrier((both, tiles[:, 0]))
    corner = jnp.where(my_col == 0, both[cols], both[0])
    got = [corner]
    for shift in range(1, grid_cols):
        got.append(lax.ppermute(corner, "col", [(0, shift), (1, (1 + shift) % grid_cols)]))
    below = lax.select_n(my_col, *got)
    right = lax.select_n((my_col + grid_cols - 1) % grid_cols, *got)
    corners = jnp.stack([right, below])
    size = lax.axis_size("row_1")
    corners = gather(corners, "row_1", size, lax.axis_index("row_1"))
    size = lax.axis_size("row_0")
    corners = gather(corners, "row_0", size, lax.axis_index("row_0"))
    corners = corners.reshape(grid_rows, 2, piece, block).transpose(1, 0, 2, 3).reshape(2, block, block)

    panels = jnp.stack(spread(panel.reshape(grid_cols, share, block), "col", grid_cols, my_col))
    got = [panels]
    for shift in range(1, grid_cols):
        got.append(lax.ppermute(panels, "col", [(i, (i + shift) % grid_cols) for i in range(grid_cols)]))
    panels = jnp.stack(got)

    base = pl.pallas_call(
        weigh_kernel,
        out_shape=jax.ShapeDtypeStruct((cols, 8, block), F32),
        grid=(cols,),
        in_specs=[pl.BlockSpec((8, rows), lambda c: (0, 0)), column_of_tiles],
        out_specs=one_check,
        cost_estimate=pl.CostEstimate(flops=64 * tiles.size, bytes_accessed=2 * tiles.size, transcendentals=0),
        name="weigh",
    )(weights, tiles)

    full = lambda *shape: pl.BlockSpec(shape, lambda j, *_: (0,) * len(shape))
    shared = pl.BlockSpec((1, share, block), lambda j, info: (j, 0, 0))
    left0, left1, sums = pl.pallas_call(
        left_kernel,
        out_shape=(
            jax.ShapeDtypeStruct((grid_cols, share, block), BF16),
            jax.ShapeDtypeStruct((grid_cols, share, block), BF16),
            jax.ShapeDtypeStruct((2, 8, block), F32),
        ),
        grid_spec=pltpu.PrefetchScalarGridSpec(
            num_scalar_prefetch=1,
            grid=(grid_cols,),
            in_specs=[
                pl.BlockSpec((1, 2, share, block), lambda j, info: (lax.rem(info[0] - j + grid_cols, grid_cols), 0, 0, 0)),
                full(block, block),
                full(2, block, block),
                pl.BlockSpec((1, 8, share), lambda j, info: (j, 0, 0)),
            ],
            out_specs=(shared, shared, full(2, 8, block)),
        ),
        cost_estimate=pl.CostEstimate(flops=6 * rows * block * block, bytes_accessed=12 * rows * block, transcendentals=0),
        name="left",
    )(info, panels, corners[0], multiplier, weights.reshape(8, grid_cols, share).transpose(1, 0, 2))
    left0, left1 = left0.reshape(rows, block), left1.reshape(rows, block)
    second_left = jnp.dot(corners[1], multiplier[0], preferred_element_type=F32).astype(BF16)

    own = jnp.concatenate([base[:, 0], sums[:, 0]], axis=0)
    total = own
    for mask in (1, 2, 4, 8):
        total = total + lax.ppermute(total, ROW, [(i, i ^ mask) for i in range(grid_rows)])
    pair = jnp.pad(jnp.stack([own, total], axis=1), ((0, 0), (0, 6), (0, 0)))

    whole = lambda *shape: pl.BlockSpec(shape, lambda c: (0,) * len(shape))
    out, checks = pl.pallas_call(
        trail_kernel,
        out_shape=(jax.ShapeDtypeStruct(tiles.shape, BF16), jax.ShapeDtypeStruct((cols, 8, block), F32)),
        grid=(cols,),
        in_specs=[
            smem,
            whole(rows, block),
            whole(rows, block),
            whole(block, block),
            whole(2, 8, block),
            pl.BlockSpec((grid_rows, 1, piece, block), lambda c: (0, c, 0, 0)),
            pl.BlockSpec((grid_rows, 1, piece, block), lambda c: (0, c + cols, 0, 0)),
            one_check,
            column_of_tiles,
        ],
        out_specs=(column_of_tiles, one_check),
        cost_estimate=pl.CostEstimate(flops=5 * rows * block * block * cols, bytes_accessed=4 * tiles.size, transcendentals=0),
        name="trail",
    )(info, left0, left1, second_left, pair[cols:], upper, upper, pair[:cols], tiles)
    return out.transpose(0, 2, 1, 3), checks[None, :, 0], checks[:, 1]


def solution(mesh):
    split = Mesh(mesh.devices.reshape(4, 4, mesh.shape["col"]), ("row_0", "row_1", "col"))
    in_specs = (P(None, ROW, None, "col"), P(), P(None, ROW))
    out_specs = (P(None, ROW, None, "col"), P(ROW, None, "col"), P(None, "col"))
    return jax.shard_map(local, mesh=split, in_specs=in_specs, out_specs=out_specs, check_vma=False)
```

```python
import jax
import jax.numpy as jnp
from jax import lax
from jax.experimental import pallas as pl
from jax.experimental.pallas import tpu as pltpu
from jax.sharding import Mesh
from jax.sharding import PartitionSpec as P

ROW = ("row_0", "row_1")
F32, BF16 = jnp.float32, jnp.bfloat16


def shifts(axis, pieces, pairs):
    return [pieces[0]] + [lax.ppermute(p, axis, pairs(s)) for s, p in enumerate(pieces) if s > 0]


def from_two(got, place):
    size = len(got)
    return lax.select_n(place, *got), lax.select_n((place + size - 1) % size, *got)


def bands_kernel(info_ref, early_ref, late_ref, *out_refs):
    parts = early_ref.shape[2]
    for s in range(parts):
        out_refs[s][:, 0] = early_ref[0, :, lax.rem(info_ref[2] + s, parts)]
        out_refs[parts + s][:, 0] = late_ref[0, s]


def panels_kernel(info_ref, panel_ref, *out_refs):
    parts = len(out_refs)
    for s in range(parts):
        out_refs[s][...] = panel_ref[:, 0, lax.rem(info_ref[0] + s, parts)]


def in_three(rows):
    high = rows.astype(BF16).astype(F32)
    middle = (rows - high).astype(BF16).astype(F32)
    low = rows - high - middle
    return jnp.concatenate([high, middle, low, jnp.zeros_like(rows)], axis=0).astype(BF16)


def times_rows(rows, right):
    product = jnp.dot(in_three(rows), right, preferred_element_type=F32)
    return product[0:8] + product[8:16] + product[16:24]


def weigh_kernel(weight_ref, tile_ref, out_ref):
    block_rows, _, width, _ = tile_ref.shape
    tile = tile_ref[...].reshape(block_rows * width, width)
    out_ref[0] = times_rows(weight_ref[...], tile)


def left_kernel(info_ref, panel_ref, corner_ref, multiplier_ref, weight_ref, left0_ref, left1_ref, sum_ref):
    step = pl.program_id(0)
    _, _, block_rows, piece, width = panel_ref.shape
    share = block_rows * piece
    row = lax.broadcasted_iota(jnp.int32, (share, width), 0)
    my_row = info_ref[1]

    def keep(value, pivot):
        return jnp.where((row < piece) & (my_row <= pivot), jnp.zeros_like(value), value)

    column0 = panel_ref[0, 0].reshape(share, width)
    column1 = panel_ref[0, 1].reshape(share, width)
    left0 = jnp.dot(column0, multiplier_ref[0], preferred_element_type=F32)
    left0 = keep(left0, 0).astype(BF16)
    column = jnp.dot(left0, corner_ref[...], preferred_element_type=F32)
    column = (column1.astype(F32) - column).astype(BF16)
    left1 = jnp.dot(column, multiplier_ref[1], preferred_element_type=F32)
    left1 = keep(left1, 1).astype(BF16)
    left0_ref[:, 0] = left0.reshape(block_rows, piece, width)
    left1_ref[:, 0] = left1.reshape(block_rows, piece, width)

    @pl.when(step == 0)
    def _():
        sum_ref[...] = jnp.zeros_like(sum_ref)

    sum_ref[0] += times_rows(weight_ref[0], left0)
    sum_ref[1] += times_rows(weight_ref[0], left1)


def trail_kernel(
    info_ref, left0_ref, left1_ref, second_ref, sums_ref, upper_ref, band_ref, base_ref, tile_ref, out_ref, check_ref
):
    width = second_ref.shape[0]
    first = pl.program_id(0) == 0
    my_col, my_row = info_ref[0], info_ref[1]
    upper0 = upper_ref[...].reshape(width, width)
    upper0 = jnp.where(first & (my_col == 0), jnp.zeros_like(upper0), upper0)
    upper1 = band_ref[...].reshape(width, width).astype(F32)
    upper1 = (upper1 - jnp.dot(second_ref[...], upper0, preferred_element_type=F32)).astype(BF16)
    upper1 = jnp.where(first & (my_col < 2), jnp.zeros_like(upper1), upper1)
    check_ref[0] = base_ref[0] - times_rows(sums_ref[0], upper0) - times_rows(sums_ref[1], upper1)
    for a in range(tile_ref.shape[0]):
        rows = slice(a * width, (a + 1) * width)
        product = jnp.dot(left0_ref[rows, :], upper0, preferred_element_type=F32)
        tile = (tile_ref[a, 0].astype(F32) - product).astype(BF16)
        product = jnp.dot(left1_ref[rows, :], upper1, preferred_element_type=F32)
        out_ref[a, 0] = (tile.astype(F32) - product).astype(BF16)
        for pivot, left_ref in enumerate((left0_ref, left1_ref)):
            below = True if a > 0 else my_row > pivot

            @pl.when(first & (my_col == pivot) & below)
            def _():
                out_ref[a, 0] = left_ref[rows, :]


def eliminate(matrix, multiplier, checksum_weight):
    block_rows, block, cols, _ = matrix.shape
    grid_rows, grid_cols = lax.axis_size(ROW), lax.axis_size("col")
    my_row, my_col = lax.axis_index(ROW), lax.axis_index("col")
    info = jnp.stack([my_col, my_row, lax.axis_index("row_1")]).astype(jnp.int32)
    tiles = matrix.transpose(0, 2, 1, 3)
    rows, piece, share = block_rows * block, block // grid_rows, block_rows * block // grid_cols
    weights = jnp.pad(checksum_weight.reshape(1, rows), ((0, 7), (0, 0)))
    smem = pl.BlockSpec(memory_space=pltpu.SMEM)
    column_of_tiles = pl.BlockSpec((block_rows, 1, block, block), lambda c: (0, c, 0, 0))
    one_check = pl.BlockSpec((1, 8, block), lambda c: (c, 0, 0))

    half, sides = cols // 2, lax.axis_size("row_1")
    my_y, my_z = lax.axis_index("row_0"), lax.axis_index("row_1")

    tall = tiles.reshape(block_rows * cols, sides, sides, piece, block)
    cell = jax.ShapeDtypeStruct((sides, half, piece, block), BF16)
    cells = pl.pallas_call(
        bands_kernel,
        out_shape=(cell,) * (2 * sides),
        grid=(half,),
        in_specs=[
            smem,
            pl.BlockSpec((1, sides, sides, piece, block), lambda c: (c, 0, 0, 0, 0)),
            pl.BlockSpec((1, sides, sides, piece, block), lambda c: (c + half, 0, 0, 0, 0)),
        ],
        out_specs=(pl.BlockSpec((sides, 1, piece, block), lambda c: (0, c, 0, 0)),) * (2 * sides),
        cost_estimate=pl.CostEstimate(flops=cols * block * block, bytes_accessed=4 * cols * block * block, transcendentals=0),
        name="bands",
    )(info, tall, tall)
    early = shifts(ROW, cells[:sides], lambda s: [(0, s), (1, (1 + s) % sides)])
    late = shifts(ROW, cells[sides:], lambda s: [(0, sides * s), (1, sides * s + 1)])

    strip = block // grid_cols
    deep = tiles.reshape(block_rows, cols, grid_cols, strip, block)
    cell = jax.ShapeDtypeStruct((block_rows, strip, block), BF16)
    cells = pl.pallas_call(
        panels_kernel,
        out_shape=(cell,) * grid_cols,
        grid=(1,),
        in_specs=[smem, pl.BlockSpec((block_rows, 1, grid_cols, strip, block), lambda j: (0, 0, 0, 0, 0))],
        out_specs=(pl.BlockSpec((block_rows, strip, block), lambda j: (0, 0, 0)),) * grid_cols,
        cost_estimate=pl.CostEstimate(flops=rows * block, bytes_accessed=4 * rows * block, transcendentals=0),
        name="panels",
    )(info, deep)
    panels = shifts("col", cells, lambda s: [(0, s), (1, (1 + s) % grid_cols)])
    panel0, panel1 = from_two(panels, my_col)

    early = jnp.stack(from_two(early, my_z), axis=1)
    early = shifts(ROW, list(early), lambda s: [(z, sides * s + z) for z in range(sides)])
    early = lax.select_n(my_y, *early)
    late = lax.select_n(my_y, *late)
    late = jnp.where(my_z == 1, jnp.roll(late, -1, axis=0), late)
    late = shifts(
        ROW,
        list(late),
        lambda s: [(sides * y + r, sides * y + (r + s) % sides) for y in range(sides) for r in (0, 1)],
    )
    late = jnp.stack(from_two(late, my_z))
    upper = lax.all_gather(jnp.concatenate([early, late], axis=1), ROW)
    upper = upper.reshape(grid_rows, 2 * cols, piece, block)

    corner = jnp.where(my_row == 1, panel0[0], panel1[0])
    corner = shifts("row_1", [corner] * sides, lambda s: [(0, s), (1, (1 + s) % sides)])
    corner = jnp.stack(from_two(corner, my_z))
    corner = shifts("row_0", [corner] * sides, lambda s: [(0, s)])
    corner = lax.select_n(my_y, *corner)
    around = lambda s: [(i, (i + s) % grid_cols) for i in range(grid_cols)]
    corner = shifts("col", [corner] * grid_cols, around)
    ordered = corner[::-1]
    ordered = lax.dynamic_slice_in_dim(jnp.stack(ordered + ordered[:-1]), grid_cols - 1 - my_col, grid_cols, 0)
    corners = ordered.transpose(1, 0, 2, 3).reshape(2, block, block)

    packed = jnp.stack([panel0, panel1])
    packed = jnp.stack(shifts("col", [packed] * grid_cols, around))

    base = pl.pallas_call(
        weigh_kernel,
        out_shape=jax.ShapeDtypeStruct((cols, 8, block), F32),
        grid=(cols,),
        in_specs=[pl.BlockSpec((8, rows), lambda c: (0, 0)), column_of_tiles],
        out_specs=one_check,
        cost_estimate=pl.CostEstimate(flops=64 * tiles.size, bytes_accessed=2 * tiles.size, transcendentals=0),
        name="weigh",
    )(weights, tiles)

    strips = weights.reshape(8, block_rows, grid_cols, strip).transpose(2, 0, 1, 3).reshape(grid_cols, 8, share)
    full = lambda *shape: pl.BlockSpec(shape, lambda j, *_: (0,) * len(shape))
    shared = pl.BlockSpec((block_rows, 1, strip, block), lambda j, info: (0, j, 0, 0))
    left_shape = jax.ShapeDtypeStruct((block_rows, grid_cols, strip, block), BF16)
    left0, left1, sums = pl.pallas_call(
        left_kernel,
        out_shape=(
            left_shape,
            left_shape,
            jax.ShapeDtypeStruct((2, 8, block), F32),
        ),
        grid_spec=pltpu.PrefetchScalarGridSpec(
            num_scalar_prefetch=1,
            grid=(grid_cols,),
            in_specs=[
                pl.BlockSpec((1, 2, block_rows, strip, block), lambda j, info: (lax.rem(info[0] - j + grid_cols, grid_cols), 0, 0, 0, 0)),
                full(block, block),
                full(2, block, block),
                pl.BlockSpec((1, 8, share), lambda j, info: (j, 0, 0)),
            ],
            out_specs=(shared, shared, full(2, 8, block)),
        ),
        cost_estimate=pl.CostEstimate(flops=6 * rows * block * block, bytes_accessed=12 * rows * block, transcendentals=0),
        name="left",
    )(info, packed, corners[0], multiplier, strips)
    left0, left1 = left0.reshape(rows, block), left1.reshape(rows, block)
    second_left = jnp.dot(corners[1], multiplier[0], preferred_element_type=F32).astype(BF16)

    own = jnp.concatenate([base[:, 0], sums[:, 0]], axis=0)
    total = own
    for mask in (1, 2, 4, 8):
        total = total + lax.ppermute(total, ROW, [(i, i ^ mask) for i in range(grid_rows)])
    pair = jnp.pad(jnp.stack([own, total], axis=1), ((0, 0), (0, 6), (0, 0)))

    whole = lambda *shape: pl.BlockSpec(shape, lambda c: (0,) * len(shape))
    out, checks = pl.pallas_call(
        trail_kernel,
        out_shape=(jax.ShapeDtypeStruct(tiles.shape, BF16), jax.ShapeDtypeStruct((cols, 8, block), F32)),
        grid=(cols,),
        in_specs=[
            smem,
            whole(rows, block),
            whole(rows, block),
            whole(block, block),
            whole(2, 8, block),
            pl.BlockSpec((grid_rows, 1, piece, block), lambda c: (0, c, 0, 0)),
            pl.BlockSpec((grid_rows, 1, piece, block), lambda c: (0, c + cols, 0, 0)),
            one_check,
            column_of_tiles,
        ],
        out_specs=(column_of_tiles, one_check),
        cost_estimate=pl.CostEstimate(flops=5 * rows * block * block * cols, bytes_accessed=4 * tiles.size, transcendentals=0),
        name="trail",
    )(info, left0, left1, second_left, pair[cols:], upper, upper, pair[:cols], tiles)
    return out.transpose(0, 2, 1, 3), checks[None, :, 0], checks[:, 1]


def solution(mesh):
    split = Mesh(mesh.devices.reshape(4, 4, mesh.shape["col"]), ("row_0", "row_1", "col"))
    in_specs = (P(None, ROW, None, "col"), P(), P(None, ROW))
    out_specs = (P(None, ROW, None, "col"), P(ROW, None, "col"), P(None, "col"))
    return jax.shard_map(eliminate, mesh=split, in_specs=in_specs, out_specs=out_specs, check_vma=False)
```

```python
import functools

import jax
import jax.numpy as jnp
from jax import lax
from jax.experimental import pallas as pl
from jax.experimental.pallas import tpu as pltpu
from jax.sharding import Mesh
from jax.sharding import PartitionSpec as P

ROW = ("row_0", "row_1")
F32, BF16 = jnp.float32, jnp.bfloat16


def shifts(axis, pieces, pairs):
    return [pieces[0]] + [lax.ppermute(p, axis, pairs(s)) for s, p in enumerate(pieces) if s > 0]


def from_two(got, place):
    size = len(got)
    return lax.select_n(place, *got), lax.select_n((place + size - 1) % size, *got)


def bands_kernel(info_ref, early_ref, late_ref, *out_refs):
    parts = early_ref.shape[2]
    for s in range(parts):
        out_refs[s][:, 0] = early_ref[0, :, lax.rem(info_ref[2] + s, parts)]
        out_refs[parts + s][:, 0] = late_ref[0, s]


def panels_kernel(info_ref, panel_ref, *out_refs):
    parts = len(out_refs)
    for s in range(parts):
        out_refs[s][...] = panel_ref[:, 0, lax.rem(info_ref[0] + s, parts)]


def in_three(rows):
    high = rows.astype(BF16).astype(F32)
    middle = (rows - high).astype(BF16).astype(F32)
    low = rows - high - middle
    return jnp.concatenate([high, middle, low, jnp.zeros_like(rows)], axis=0).astype(BF16)


def times_rows(rows, right):
    product = jnp.dot(in_three(rows), right, preferred_element_type=F32)
    return product[0:8] + product[8:16] + product[16:24]


def weigh_kernel(weight_ref, tile_ref, out_ref):
    block_rows, _, width, _ = tile_ref.shape
    tile = tile_ref[...].reshape(block_rows * width, width)
    out_ref[0] = times_rows(weight_ref[...], tile)


def left_kernel(info_ref, panel_ref, corner_ref, multiplier_ref, weight_ref, left0_ref, left1_ref, sum_ref):
    block_rows, width = left0_ref.shape[0] // corner_ref.shape[0], corner_ref.shape[0]
    strips, _, _, _, _ = panel_ref.shape

    def column(step):
        parts = [panel_ref[j, step, a] for a in range(block_rows) for j in range(strips)]
        return jnp.concatenate(parts, axis=0)

    def finish(step, factor, left_ref):
        left = jnp.dot(factor, multiplier_ref[step], preferred_element_type=F32).astype(BF16)
        left_ref[...] = left

        @pl.when(info_ref[1] <= step)
        def _():
            left_ref[:width] = jnp.zeros((width, width), BF16)

        sum_ref[step] = times_rows(weight_ref[...], left_ref[...])

    finish(0, column(0), left0_ref)
    update = jnp.dot(left0_ref[...], corner_ref[...], preferred_element_type=F32)
    finish(1, (column(1).astype(F32) - update).astype(BF16), left1_ref)


def trail_kernel(
    info_ref, left0_ref, left1_ref, second_ref, sums_ref, upper_ref, band_ref, base_ref, tile_ref, out_ref, check_ref
):
    width = second_ref.shape[0]
    first = pl.program_id(0) == 0
    my_col, my_row = info_ref[0], info_ref[1]
    upper0 = upper_ref[...].reshape(width, width)
    upper0 = jnp.where(first & (my_col == 0), jnp.zeros_like(upper0), upper0)
    upper1 = band_ref[...].reshape(width, width).astype(F32)
    upper1 = (upper1 - jnp.dot(second_ref[...], upper0, preferred_element_type=F32)).astype(BF16)
    upper1 = jnp.where(first & (my_col < 2), jnp.zeros_like(upper1), upper1)
    check_ref[0] = base_ref[0] - times_rows(sums_ref[0], upper0) - times_rows(sums_ref[1], upper1)
    for a in range(tile_ref.shape[0]):
        rows = slice(a * width, (a + 1) * width)
        tile = tile_ref[a, 0].astype(F32) - jnp.dot(left0_ref[rows, :], upper0, preferred_element_type=F32)
        tile = tile.astype(BF16).astype(F32)
        tile = tile - jnp.dot(left1_ref[rows, :], upper1, preferred_element_type=F32)
        out_ref[a, 0] = tile.astype(BF16)
    for a in range(tile_ref.shape[0]):
        for pivot, left_ref in enumerate((left0_ref, left1_ref)):
            below = True if a > 0 else my_row > pivot

            @pl.when(first & (my_col == pivot) & below)
            def _():
                out_ref[a, 0] = left_ref[a * width : (a + 1) * width, :]


def eliminate(matrix, multiplier, checksum_weight):
    block_rows, block, cols, _ = matrix.shape
    grid_rows, grid_cols = lax.axis_size(ROW), lax.axis_size("col")
    my_row, my_col = lax.axis_index(ROW), lax.axis_index("col")
    info = jnp.stack([my_col, my_row, lax.axis_index("row_1")]).astype(jnp.int32)
    tiles = matrix.transpose(0, 2, 1, 3)
    rows, piece = block_rows * block, block // grid_rows
    weights = jnp.pad(checksum_weight.reshape(1, rows), ((0, 7), (0, 0)))
    smem = pl.BlockSpec(memory_space=pltpu.SMEM)
    column_of_tiles = pl.BlockSpec((block_rows, 1, block, block), lambda c: (0, c, 0, 0))
    one_check = pl.BlockSpec((1, 8, block), lambda c: (c, 0, 0))

    half, sides = cols // 2, lax.axis_size("row_1")
    my_y, my_z = lax.axis_index("row_0"), lax.axis_index("row_1")

    strip = block // grid_cols
    deep = tiles.reshape(block_rows, cols, grid_cols, strip, block)
    cell = jax.ShapeDtypeStruct((block_rows, strip, block), BF16)
    cells = pl.pallas_call(
        panels_kernel,
        out_shape=(cell,) * grid_cols,
        grid=(1,),
        in_specs=[smem, pl.BlockSpec((block_rows, 1, grid_cols, strip, block), lambda j: (0, 0, 0, 0, 0))],
        out_specs=(pl.BlockSpec((block_rows, strip, block), lambda j: (0, 0, 0)),) * grid_cols,
        cost_estimate=pl.CostEstimate(flops=rows * block, bytes_accessed=4 * rows * block, transcendentals=0),
        name="panels",
    )(info, deep)
    panels = shifts("col", cells, lambda s: [(0, s), (1, (1 + s) % grid_cols)])
    panel0, panel1 = from_two(panels, my_col)
    panels = lax.all_gather(jnp.stack([panel0, panel1]), "col")

    tall = tiles.reshape(block_rows * cols, sides, sides, piece, block)
    cell = jax.ShapeDtypeStruct((sides, half, piece, block), BF16)
    cells = pl.pallas_call(
        bands_kernel,
        out_shape=(cell,) * (2 * sides),
        grid=(half,),
        in_specs=[
            smem,
            pl.BlockSpec((1, sides, sides, piece, block), lambda c: (c, 0, 0, 0, 0)),
            pl.BlockSpec((1, sides, sides, piece, block), lambda c: (c + half, 0, 0, 0, 0)),
        ],
        out_specs=(pl.BlockSpec((sides, 1, piece, block), lambda c: (0, c, 0, 0)),) * (2 * sides),
        cost_estimate=pl.CostEstimate(flops=cols * block * block, bytes_accessed=4 * cols * block * block, transcendentals=0),
        name="bands",
    )(info, tall, tall)
    early = shifts(ROW, cells[:sides], lambda s: [(0, s), (1, (1 + s) % sides)])
    late = shifts(ROW, cells[sides:], lambda s: [(0, sides * s), (1, sides * s + 1)])

    early = jnp.stack(from_two(early, my_z), axis=1)
    early = shifts(ROW, list(early), lambda s: [(z, sides * s + z) for z in range(sides)])
    early = lax.select_n(my_y, *early)
    late = lax.select_n(my_y, *late)
    late = jnp.where(my_z == 1, jnp.roll(late, -1, axis=0), late)
    late = shifts(
        ROW,
        list(late),
        lambda s: [(sides * y + r, sides * y + (r + s) % sides) for y in range(sides) for r in (0, 1)],
    )
    late = jnp.stack(from_two(late, my_z))
    upper = lax.all_gather(jnp.concatenate([early, late], axis=1), ROW)
    upper = upper.reshape(grid_rows, 2 * cols, piece, block)

    corner = jnp.where(my_row == 1, panel0[0], panel1[0])
    corner = shifts("row_1", [corner] * sides, lambda s: [(0, s), (1, (1 + s) % sides)])
    corner = jnp.stack(from_two(corner, my_z))
    corner = shifts("row_0", [corner] * sides, lambda s: [(0, s)])
    corner = lax.select_n(my_y, *corner)
    around = lambda s: [(i, (i + s) % grid_cols) for i in range(grid_cols)]
    corner = shifts("col", [corner] * grid_cols, around)
    ordered = corner[::-1]
    ordered = lax.dynamic_slice_in_dim(jnp.stack(ordered + ordered[:-1]), grid_cols - 1 - my_col, grid_cols, 0)
    corners = ordered.transpose(1, 0, 2, 3).reshape(2, block, block)

    base = pl.pallas_call(
        weigh_kernel,
        out_shape=jax.ShapeDtypeStruct((cols, 8, block), F32),
        grid=(cols,),
        in_specs=[pl.BlockSpec((8, rows), lambda c: (0, 0)), column_of_tiles],
        out_specs=one_check,
        cost_estimate=pl.CostEstimate(flops=64 * tiles.size, bytes_accessed=2 * tiles.size, transcendentals=0),
        name="weigh",
    )(weights, tiles)

    left0, left1, sums = pl.pallas_call(
        left_kernel,
        out_shape=(
            jax.ShapeDtypeStruct((rows, block), BF16),
            jax.ShapeDtypeStruct((rows, block), BF16),
            jax.ShapeDtypeStruct((2, 8, block), F32),
        ),
        in_specs=[smem] + [pl.BlockSpec(memory_space=pltpu.VMEM)] * 4,
        out_specs=(pl.BlockSpec(memory_space=pltpu.VMEM),) * 3,
        cost_estimate=pl.CostEstimate(flops=6 * rows * block * block, bytes_accessed=12 * rows * block, transcendentals=0),
        compiler_params=pltpu.CompilerParams(vmem_limit_bytes=24 << 20),
        name="left",
    )(info, panels, corners[0], multiplier, weights)
    second_left = jnp.dot(corners[1], multiplier[0], preferred_element_type=F32).astype(BF16)

    own = jnp.concatenate([base[:, 0], sums[:, 0]], axis=0)
    total = own
    for axis in ("row_1", "row_0"):
        around = lambda s: [(i, (i + s) % sides) for i in range(sides)]
        total = functools.reduce(jnp.add, shifts(axis, [total] * sides, around))
    pair = jnp.pad(jnp.stack([own, total], axis=1), ((0, 0), (0, 6), (0, 0)))

    whole = lambda *shape: pl.BlockSpec(shape, lambda c: (0,) * len(shape))
    out, checks = pl.pallas_call(
        trail_kernel,
        out_shape=(jax.ShapeDtypeStruct(tiles.shape, BF16), jax.ShapeDtypeStruct((cols, 8, block), F32)),
        grid=(cols,),
        in_specs=[
            smem,
            whole(rows, block),
            whole(rows, block),
            whole(block, block),
            whole(2, 8, block),
            pl.BlockSpec((grid_rows, 1, piece, block), lambda c: (0, c, 0, 0)),
            pl.BlockSpec((grid_rows, 1, piece, block), lambda c: (0, c + cols, 0, 0)),
            one_check,
            column_of_tiles,
        ],
        out_specs=(column_of_tiles, one_check),
        cost_estimate=pl.CostEstimate(flops=5 * rows * block * block * cols, bytes_accessed=4 * tiles.size, transcendentals=0),
        name="trail",
    )(info, left0, left1, second_left, pair[cols:], upper, upper, pair[:cols], tiles)
    return out.transpose(0, 2, 1, 3), checks[None, :, 0], checks[:, 1]


def solution(mesh):
    split = Mesh(mesh.devices.reshape(4, 4, mesh.shape["col"]), ("row_0", "row_1", "col"))
    in_specs = (P(None, ROW, None, "col"), P(), P(None, ROW))
    out_specs = (P(None, ROW, None, "col"), P(ROW, None, "col"), P(None, "col"))
    return jax.shard_map(eliminate, mesh=split, in_specs=in_specs, out_specs=out_specs, check_vma=False)
```

```python
import functools

import jax
import jax.numpy as jnp
from jax import lax
from jax.experimental import pallas as pl
from jax.experimental.pallas import tpu as pltpu
from jax.sharding import Mesh
from jax.sharding import PartitionSpec as P

ROW = ("row_0", "row_1")
F32, BF16 = jnp.float32, jnp.bfloat16


def shifts(axis, pieces, pairs):
    return [pieces[0]] + [lax.ppermute(p, axis, pairs(s)) for s, p in enumerate(pieces) if s > 0]


def from_two(got, place):
    size = len(got)
    return lax.select_n(place, *got), lax.select_n((place + size - 1) % size, *got)


def bands_kernel(tile_ref, out_ref):
    out_ref[:, 0] = tile_ref[0]


def panels_kernel(info_ref, panel_ref, *out_refs):
    parts = len(out_refs)
    for s in range(parts):
        out_refs[s][...] = panel_ref[:, 0, lax.rem(info_ref[0] + s, parts)]


def in_three(rows):
    high = rows.astype(BF16).astype(F32)
    middle = (rows - high).astype(BF16).astype(F32)
    low = rows - high - middle
    return jnp.concatenate([high, middle, low, jnp.zeros_like(rows)], axis=0).astype(BF16)


def times_rows(rows, right):
    product = jnp.dot(in_three(rows), right, preferred_element_type=F32)
    return product[0:8] + product[8:16] + product[16:24]


def weigh_kernel(weight_ref, tile_ref, out_ref):
    block_rows, _, width, _ = tile_ref.shape
    tile = tile_ref[...].reshape(block_rows * width, width)
    out_ref[0] = times_rows(weight_ref[...], tile)


def left_kernel(info_ref, panel_ref, corner_ref, multiplier_ref, weight_ref, left0_ref, left1_ref, sum_ref):
    block_rows, width = left0_ref.shape[0] // corner_ref.shape[0], corner_ref.shape[0]
    strips, _, _, _, _ = panel_ref.shape

    def column(step):
        parts = [panel_ref[j, step, a] for a in range(block_rows) for j in range(strips)]
        return jnp.concatenate(parts, axis=0)

    def finish(step, factor, left_ref):
        left = jnp.dot(factor, multiplier_ref[step], preferred_element_type=F32).astype(BF16)
        left_ref[...] = left

        @pl.when(info_ref[1] <= step)
        def _():
            left_ref[:width] = jnp.zeros((width, width), BF16)

        sum_ref[step] = times_rows(weight_ref[...], left_ref[...])

    finish(0, column(0), left0_ref)
    update = jnp.dot(left0_ref[...], corner_ref[...], preferred_element_type=F32)
    finish(1, (column(1).astype(F32) - update).astype(BF16), left1_ref)


def trail_kernel(
    info_ref, left0_ref, left1_ref, second_ref, sums_ref, upper_ref, band_ref, base_ref, tile_ref, out_ref, check_ref
):
    width = second_ref.shape[0]
    first = pl.program_id(0) == 0
    my_col, my_row = info_ref[0], info_ref[1]
    upper0 = upper_ref[...].reshape(width, width)
    upper0 = jnp.where(first & (my_col == 0), jnp.zeros_like(upper0), upper0)
    upper1 = band_ref[...].reshape(width, width).astype(F32)
    upper1 = (upper1 - jnp.dot(second_ref[...], upper0, preferred_element_type=F32)).astype(BF16)
    upper1 = jnp.where(first & (my_col < 2), jnp.zeros_like(upper1), upper1)
    check_ref[0] = base_ref[0] - times_rows(sums_ref[0], upper0) - times_rows(sums_ref[1], upper1)
    for a in range(tile_ref.shape[0]):
        rows = slice(a * width, (a + 1) * width)
        tile = tile_ref[a, 0].astype(F32) - jnp.dot(left0_ref[rows, :], upper0, preferred_element_type=F32)
        tile = tile.astype(BF16).astype(F32)
        tile = tile - jnp.dot(left1_ref[rows, :], upper1, preferred_element_type=F32)
        out_ref[a, 0] = tile.astype(BF16)
    for a in range(tile_ref.shape[0]):
        for pivot, left_ref in enumerate((left0_ref, left1_ref)):
            below = True if a > 0 else my_row > pivot

            @pl.when(first & (my_col == pivot) & below)
            def _():
                out_ref[a, 0] = left_ref[a * width : (a + 1) * width, :]


def eliminate(matrix, multiplier, checksum_weight):
    block_rows, block, cols, _ = matrix.shape
    grid_rows, grid_cols = lax.axis_size(ROW), lax.axis_size("col")
    my_row, my_col = lax.axis_index(ROW), lax.axis_index("col")
    info = jnp.stack([my_col, my_row, lax.axis_index("row_1")]).astype(jnp.int32)
    tiles = matrix.transpose(0, 2, 1, 3)
    rows, piece = block_rows * block, block // grid_rows
    weights = jnp.pad(checksum_weight.reshape(1, rows), ((0, 7), (0, 0)))
    smem = pl.BlockSpec(memory_space=pltpu.SMEM)
    column_of_tiles = pl.BlockSpec((block_rows, 1, block, block), lambda c: (0, c, 0, 0))
    one_check = pl.BlockSpec((1, 8, block), lambda c: (c, 0, 0))

    sides = lax.axis_size("row_1")
    my_y, my_z = lax.axis_index("row_0"), lax.axis_index("row_1")

    bands = pl.pallas_call(
        bands_kernel,
        out_shape=jax.ShapeDtypeStruct((grid_rows, cols, piece, block), BF16),
        grid=(cols,),
        in_specs=[pl.BlockSpec((1, grid_rows, piece, block), lambda c: (c, 0, 0, 0))],
        out_specs=pl.BlockSpec((grid_rows, 1, piece, block), lambda c: (0, c, 0, 0)),
        cost_estimate=pl.CostEstimate(flops=cols * block * block, bytes_accessed=4 * cols * block * block, transcendentals=0),
        name="bands",
    )(tiles.reshape(block_rows * cols, grid_rows, piece, block))
    bands = lax.all_to_all(bands, ROW, 0, 0)
    upper = lax.all_gather(bands[:2], ROW).reshape(grid_rows, 2 * cols, piece, block)

    strip = block // grid_cols
    deep = tiles.reshape(block_rows, cols, grid_cols, strip, block)
    cell = jax.ShapeDtypeStruct((block_rows, strip, block), BF16)
    cells = pl.pallas_call(
        panels_kernel,
        out_shape=(cell,) * grid_cols,
        grid=(1,),
        in_specs=[smem, pl.BlockSpec((block_rows, 1, grid_cols, strip, block), lambda j: (0, 0, 0, 0, 0))],
        out_specs=(pl.BlockSpec((block_rows, strip, block), lambda j: (0, 0, 0)),) * grid_cols,
        cost_estimate=pl.CostEstimate(flops=rows * block, bytes_accessed=4 * rows * block, transcendentals=0),
        name="panels",
    )(info, deep)
    panels = shifts("col", cells, lambda s: [(0, s), (1, (1 + s) % grid_cols)])
    panel0, panel1 = from_two(panels, my_col)
    panels = lax.all_gather(jnp.stack([panel0, panel1]), "col")

    corner = jnp.where(my_row == 1, panel0[0], panel1[0])
    corner = shifts("row_1", [corner] * sides, lambda s: [(0, s), (1, (1 + s) % sides)])
    corner = jnp.stack(from_two(corner, my_z))
    corner = shifts("row_0", [corner] * sides, lambda s: [(0, s)])
    corner = lax.select_n(my_y, *corner)
    around = lambda s: [(i, (i + s) % grid_cols) for i in range(grid_cols)]
    corner = shifts("col", [corner] * grid_cols, around)
    ordered = corner[::-1]
    ordered = lax.dynamic_slice_in_dim(jnp.stack(ordered + ordered[:-1]), grid_cols - 1 - my_col, grid_cols, 0)
    corners = ordered.transpose(1, 0, 2, 3).reshape(2, block, block)

    base = pl.pallas_call(
        weigh_kernel,
        out_shape=jax.ShapeDtypeStruct((cols, 8, block), F32),
        grid=(cols,),
        in_specs=[pl.BlockSpec((8, rows), lambda c: (0, 0)), column_of_tiles],
        out_specs=one_check,
        cost_estimate=pl.CostEstimate(flops=64 * tiles.size, bytes_accessed=2 * tiles.size, transcendentals=0),
        name="weigh",
    )(weights, tiles)

    left0, left1, sums = pl.pallas_call(
        left_kernel,
        out_shape=(
            jax.ShapeDtypeStruct((rows, block), BF16),
            jax.ShapeDtypeStruct((rows, block), BF16),
            jax.ShapeDtypeStruct((2, 8, block), F32),
        ),
        in_specs=[smem] + [pl.BlockSpec(memory_space=pltpu.VMEM)] * 4,
        out_specs=(pl.BlockSpec(memory_space=pltpu.VMEM),) * 3,
        cost_estimate=pl.CostEstimate(flops=6 * rows * block * block, bytes_accessed=12 * rows * block, transcendentals=0),
        compiler_params=pltpu.CompilerParams(vmem_limit_bytes=24 << 20),
        name="left",
    )(info, panels, corners[0], multiplier, weights)
    second_left = jnp.dot(corners[1], multiplier[0], preferred_element_type=F32).astype(BF16)

    own = jnp.concatenate([base[:, 0], sums[:, 0]], axis=0)
    total = own
    for axis in ("row_1", "row_0"):
        around = lambda s: [(i, (i + s) % sides) for i in range(sides)]
        total = functools.reduce(jnp.add, shifts(axis, [total] * sides, around))
    pair = jnp.pad(jnp.stack([own, total], axis=1), ((0, 0), (0, 6), (0, 0)))

    whole = lambda *shape: pl.BlockSpec(shape, lambda c: (0,) * len(shape))
    out, checks = pl.pallas_call(
        trail_kernel,
        out_shape=(jax.ShapeDtypeStruct(tiles.shape, BF16), jax.ShapeDtypeStruct((cols, 8, block), F32)),
        grid=(cols,),
        in_specs=[
            smem,
            whole(rows, block),
            whole(rows, block),
            whole(block, block),
            whole(2, 8, block),
            pl.BlockSpec((grid_rows, 1, piece, block), lambda c: (0, c, 0, 0)),
            pl.BlockSpec((grid_rows, 1, piece, block), lambda c: (0, c + cols, 0, 0)),
            one_check,
            column_of_tiles,
        ],
        out_specs=(column_of_tiles, one_check),
        cost_estimate=pl.CostEstimate(flops=5 * rows * block * block * cols, bytes_accessed=4 * tiles.size, transcendentals=0),
        name="trail",
    )(info, left0, left1, second_left, pair[cols:], upper, upper, pair[:cols], tiles)
    return out.transpose(0, 2, 1, 3), checks[None, :, 0], checks[:, 1]


def solution(mesh):
    split = Mesh(mesh.devices.reshape(4, 4, mesh.shape["col"]), ("row_0", "row_1", "col"))
    in_specs = (P(None, ROW, None, "col"), P(), P(None, ROW))
    out_specs = (P(None, ROW, None, "col"), P(ROW, None, "col"), P(None, "col"))
    return jax.shard_map(eliminate, mesh=split, in_specs=in_specs, out_specs=out_specs, check_vma=False)
```

```python
import functools

import jax
import jax.numpy as jnp
from jax import lax
from jax.experimental import pallas as pl
from jax.experimental.pallas import tpu as pltpu
from jax.sharding import Mesh
from jax.sharding import PartitionSpec as P

ROW = ("row_0", "row_1")
F32, BF16 = jnp.float32, jnp.bfloat16


def shifts(axis, pieces, pairs):
    return [pieces[0]] + [lax.ppermute(p, axis, pairs(s)) for s, p in enumerate(pieces) if s > 0]


def from_two(got, place):
    size = len(got)
    return lax.select_n(place, *got), lax.select_n((place + size - 1) % size, *got)


def bands_kernel(tile_ref, out_ref):
    for c in range(tile_ref.shape[0]):
        out_ref[:, c] = tile_ref[c]


def panels_kernel(info_ref, panel_ref, *out_refs):
    parts = len(out_refs)
    for s in range(parts):
        out_refs[s][...] = panel_ref[:, 0, lax.rem(info_ref[0] + s, parts)]


def in_three(rows):
    high = rows.astype(BF16).astype(F32)
    middle = (rows - high).astype(BF16).astype(F32)
    low = rows - high - middle
    return jnp.concatenate([high, middle, low, jnp.zeros_like(rows)], axis=0).astype(BF16)


def times_rows(rows, right):
    product = jnp.dot(in_three(rows), right, preferred_element_type=F32)
    return product[0:8] + product[8:16] + product[16:24]


def weigh_kernel(weight_ref, tile_ref, out_ref):
    block_rows, _, width, _ = tile_ref.shape
    tile = tile_ref[...].reshape(block_rows * width, width)
    out_ref[0] = times_rows(weight_ref[...], tile)


def left_kernel(strips, info_ref, corner_ref, multiplier_ref, weight_ref, *refs):
    panel_refs, (left0_ref, left1_ref, sum_ref) = refs[:strips], refs[strips:]
    width = corner_ref.shape[0]
    _, block_rows, strip, _ = panel_refs[0].shape
    row = lax.broadcasted_iota(jnp.int32, (block_rows * width, width), 0)

    def column(step):
        parts = [ref[step, a] for a in range(block_rows) for ref in panel_refs]
        return jnp.concatenate(parts, axis=0)

    def finish(step, factor, left_ref):
        left = jnp.dot(factor, multiplier_ref[step], preferred_element_type=F32)
        left = jnp.where((row < width) & (info_ref[1] <= step), jnp.zeros_like(left), left).astype(BF16)
        for s in range(strips):
            place = lax.rem(info_ref[0] - s + strips, strips) * strip
            for a in range(block_rows):
                at = pl.multiple_of(a * width + place, strip)
                start = (a * strips + s) * strip
                left_ref[pl.ds(at, strip), :] = left[start : start + strip]
        sum_ref[step] = times_rows(weight_ref[...], left_ref[...])
        return left

    left0 = finish(0, column(0), left0_ref)
    update = jnp.dot(left0, corner_ref[...], preferred_element_type=F32)
    finish(1, (column(1).astype(F32) - update).astype(BF16), left1_ref)


def trail_kernel(
    info_ref, left0_ref, left1_ref, second_ref, sums_ref, upper_ref, band_ref, base_ref, tile_ref, out_ref, check_ref
):
    width = second_ref.shape[0]
    first = pl.program_id(0) == 0
    my_col, my_row = info_ref[0], info_ref[1]
    upper0 = upper_ref[...].reshape(width, width)
    upper0 = jnp.where(first & (my_col == 0), jnp.zeros_like(upper0), upper0)
    upper1 = band_ref[...].reshape(width, width).astype(F32)
    upper1 = (upper1 - jnp.dot(second_ref[...], upper0, preferred_element_type=F32)).astype(BF16)
    upper1 = jnp.where(first & (my_col < 2), jnp.zeros_like(upper1), upper1)
    check_ref[0] = base_ref[0] - times_rows(sums_ref[0], upper0) - times_rows(sums_ref[1], upper1)
    for a in range(tile_ref.shape[0]):
        rows = slice(a * width, (a + 1) * width)
        tile = tile_ref[a, 0].astype(F32) - jnp.dot(left0_ref[rows, :], upper0, preferred_element_type=F32)
        tile = tile.astype(BF16).astype(F32)
        tile = tile - jnp.dot(left1_ref[rows, :], upper1, preferred_element_type=F32)
        out_ref[a, 0] = tile.astype(BF16)
    for a in range(tile_ref.shape[0]):
        for pivot, left_ref in enumerate((left0_ref, left1_ref)):
            below = True if a > 0 else my_row > pivot

            @pl.when(first & (my_col == pivot) & below)
            def _():
                out_ref[a, 0] = left_ref[a * width : (a + 1) * width, :]


def eliminate(matrix, multiplier, checksum_weight):
    block_rows, block, cols, _ = matrix.shape
    grid_rows, grid_cols = lax.axis_size(ROW), lax.axis_size("col")
    my_row, my_col = lax.axis_index(ROW), lax.axis_index("col")
    info = jnp.stack([my_col, my_row, lax.axis_index("row_1")]).astype(jnp.int32)
    tiles = matrix.transpose(0, 2, 1, 3)
    rows, piece = block_rows * block, block // grid_rows
    weights = jnp.pad(checksum_weight.reshape(1, rows), ((0, 7), (0, 0)))
    smem = pl.BlockSpec(memory_space=pltpu.SMEM)
    column_of_tiles = pl.BlockSpec((block_rows, 1, block, block), lambda c: (0, c, 0, 0))
    one_check = pl.BlockSpec((1, 8, block), lambda c: (c, 0, 0))

    sides = lax.axis_size("row_1")
    my_y, my_z = lax.axis_index("row_0"), lax.axis_index("row_1")

    bands = pl.pallas_call(
        bands_kernel,
        out_shape=jax.ShapeDtypeStruct((grid_rows, cols, piece, block), BF16),
        grid=(2,),
        in_specs=[pl.BlockSpec((cols // 2, grid_rows, piece, block), lambda c: (c, 0, 0, 0))],
        out_specs=pl.BlockSpec((grid_rows, cols // 2, piece, block), lambda c: (0, c, 0, 0)),
        cost_estimate=pl.CostEstimate(flops=cols * block * block, bytes_accessed=4 * cols * block * block, transcendentals=0),
        name="bands",
    )(tiles.reshape(block_rows * cols, grid_rows, piece, block))
    bands = lax.all_to_all(bands, ROW, 0, 0)
    upper = lax.all_gather(bands[:2], ROW).reshape(grid_rows, 2 * cols, piece, block)

    strip = block // grid_cols
    deep = tiles.reshape(block_rows, cols, grid_cols, strip, block)
    cell = jax.ShapeDtypeStruct((block_rows, strip, block), BF16)
    cells = pl.pallas_call(
        panels_kernel,
        out_shape=(cell,) * grid_cols,
        grid=(1,),
        in_specs=[smem, pl.BlockSpec((block_rows, 1, grid_cols, strip, block), lambda j: (0, 0, 0, 0, 0))],
        out_specs=(pl.BlockSpec((block_rows, strip, block), lambda j: (0, 0, 0)),) * grid_cols,
        cost_estimate=pl.CostEstimate(flops=rows * block, bytes_accessed=4 * rows * block, transcendentals=0),
        name="panels",
    )(info, deep)
    panels = shifts("col", cells, lambda s: [(0, s), (1, (1 + s) % grid_cols)])
    panel0, panel1 = from_two(panels, my_col)
    panels = jnp.stack([panel0, panel1])
    around = lambda s: [(i, (i + s) % grid_cols) for i in range(grid_cols)]
    panels = shifts("col", [panels] * grid_cols, around)

    corner = jnp.where(my_row == 1, panel0[0], panel1[0])
    corner = shifts("row_1", [corner] * sides, lambda s: [(0, s), (1, (1 + s) % sides)])
    corner = jnp.stack(from_two(corner, my_z))
    corner = shifts("row_0", [corner] * sides, lambda s: [(0, s)])
    corner = lax.select_n(my_y, *corner)
    around = lambda s: [(i, (i + s) % grid_cols) for i in range(grid_cols)]
    corner = shifts("col", [corner] * grid_cols, around)
    ordered = corner[::-1]
    ordered = lax.dynamic_slice_in_dim(jnp.stack(ordered + ordered[:-1]), grid_cols - 1 - my_col, grid_cols, 0)
    corners = ordered.transpose(1, 0, 2, 3).reshape(2, block, block)

    base = pl.pallas_call(
        weigh_kernel,
        out_shape=jax.ShapeDtypeStruct((cols, 8, block), F32),
        grid=(cols,),
        in_specs=[pl.BlockSpec((8, rows), lambda c: (0, 0)), column_of_tiles],
        out_specs=one_check,
        cost_estimate=pl.CostEstimate(flops=64 * tiles.size, bytes_accessed=2 * tiles.size, transcendentals=0),
        name="weigh",
    )(weights, tiles)

    left0, left1, sums = pl.pallas_call(
        functools.partial(left_kernel, grid_cols),
        out_shape=(
            jax.ShapeDtypeStruct((rows, block), BF16),
            jax.ShapeDtypeStruct((rows, block), BF16),
            jax.ShapeDtypeStruct((2, 8, block), F32),
        ),
        in_specs=[smem] + [pl.BlockSpec(memory_space=pltpu.VMEM)] * (3 + grid_cols),
        out_specs=(pl.BlockSpec(memory_space=pltpu.VMEM),) * 3,
        cost_estimate=pl.CostEstimate(flops=6 * rows * block * block, bytes_accessed=12 * rows * block, transcendentals=0),
        compiler_params=pltpu.CompilerParams(vmem_limit_bytes=24 << 20),
        name="left",
    )(info, corners[0], multiplier, weights, *panels)
    second_left = jnp.dot(corners[1], multiplier[0], preferred_element_type=F32).astype(BF16)

    own = jnp.concatenate([base[:, 0], sums[:, 0]], axis=0)
    total = own
    for axis in ("row_1", "row_0"):
        around = lambda s: [(i, (i + s) % sides) for i in range(sides)]
        total = functools.reduce(jnp.add, shifts(axis, [total] * sides, around))
    pair = jnp.pad(jnp.stack([own, total], axis=1), ((0, 0), (0, 6), (0, 0)))

    whole = lambda *shape: pl.BlockSpec(shape, lambda c: (0,) * len(shape))
    out, checks = pl.pallas_call(
        trail_kernel,
        out_shape=(jax.ShapeDtypeStruct(tiles.shape, BF16), jax.ShapeDtypeStruct((cols, 8, block), F32)),
        grid=(cols,),
        in_specs=[
            smem,
            whole(rows, block),
            whole(rows, block),
            whole(block, block),
            whole(2, 8, block),
            pl.BlockSpec((grid_rows, 1, piece, block), lambda c: (0, c, 0, 0)),
            pl.BlockSpec((grid_rows, 1, piece, block), lambda c: (0, c + cols, 0, 0)),
            one_check,
            column_of_tiles,
        ],
        out_specs=(column_of_tiles, one_check),
        cost_estimate=pl.CostEstimate(flops=5 * rows * block * block * cols, bytes_accessed=4 * tiles.size, transcendentals=0),
        name="trail",
    )(info, left0, left1, second_left, pair[cols:], upper, upper, pair[:cols], tiles)
    return out.transpose(0, 2, 1, 3), checks[None, :, 0], checks[:, 1]


def solution(mesh):
    split = Mesh(mesh.devices.reshape(4, 4, mesh.shape["col"]), ("row_0", "row_1", "col"))
    in_specs = (P(None, ROW, None, "col"), P(), P(None, ROW))
    out_specs = (P(None, ROW, None, "col"), P(ROW, None, "col"), P(None, "col"))
    return jax.shard_map(eliminate, mesh=split, in_specs=in_specs, out_specs=out_specs, check_vma=False)
```

```python
import functools

import jax
import jax.numpy as jnp
from jax import lax
from jax.experimental import pallas as pl
from jax.experimental.pallas import tpu as pltpu
from jax.sharding import Mesh
from jax.sharding import PartitionSpec as P

ROW = ("row_0", "row_1")
F32, BF16 = jnp.float32, jnp.bfloat16


def shifts(axis, pieces, pairs):
    return [pieces[0]] + [lax.ppermute(p, axis, pairs(s)) for s, p in enumerate(pieces) if s > 0]


def from_two(got, place):
    size = len(got)
    return lax.select_n(place, *got), lax.select_n((place + size - 1) % size, *got)


def bands_kernel(tile_ref, out_ref):
    for c in range(tile_ref.shape[0]):
        out_ref[:, c] = tile_ref[c]


def panels_kernel(info_ref, panel_ref, *out_refs):
    parts = len(out_refs)
    for s in range(parts):
        out_refs[s][...] = panel_ref[:, 0, lax.rem(info_ref[0] + s, parts)]


def in_three(rows):
    high = rows.astype(BF16).astype(F32)
    middle = (rows - high).astype(BF16).astype(F32)
    low = rows - high - middle
    return jnp.concatenate([high, middle, low, jnp.zeros_like(rows)], axis=0).astype(BF16)


def times_rows(rows, right):
    product = jnp.dot(in_three(rows), right, preferred_element_type=F32)
    return product[0:8] + product[8:16] + product[16:24]


def weigh_kernel(weight_ref, tile_ref, out_ref):
    block_rows, _, width, _ = tile_ref.shape
    tile = tile_ref[...].reshape(block_rows * width, width)
    out_ref[0] = times_rows(weight_ref[...], tile)


def left_kernel(strips, info_ref, corner_ref, multiplier_ref, weight_ref, *refs):
    panel_refs, (left0_ref, left1_ref, sum_ref) = refs[:strips], refs[strips:]
    width = corner_ref.shape[0]
    _, block_rows, strip, _ = panel_refs[0].shape
    row = lax.broadcasted_iota(jnp.int32, (block_rows * width, width), 0)

    def column(step):
        parts = [ref[step, a] for a in range(block_rows) for ref in panel_refs]
        return jnp.concatenate(parts, axis=0)

    def finish(step, factor, left_ref):
        left = jnp.dot(factor, multiplier_ref[step], preferred_element_type=F32)
        left = jnp.where((row < width) & (info_ref[1] <= step), jnp.zeros_like(left), left).astype(BF16)
        for s in range(strips):
            place = lax.rem(info_ref[0] - s + strips, strips) * strip
            for a in range(block_rows):
                at = pl.multiple_of(a * width + place, strip)
                start = (a * strips + s) * strip
                left_ref[pl.ds(at, strip), :] = left[start : start + strip]
        sum_ref[step] = times_rows(weight_ref[...], left_ref[...])
        return left

    left0 = finish(0, column(0), left0_ref)
    update = jnp.dot(left0, corner_ref[...], preferred_element_type=F32)
    finish(1, (column(1).astype(F32) - update).astype(BF16), left1_ref)


def trail_kernel(
    info_ref, left0_ref, left1_ref, second_ref, own_ref, total_ref, upper_ref, band_ref, tile_ref, out_ref, check_ref, sum_ref
):
    width = second_ref.shape[0]
    first = pl.program_id(0) == 0
    my_col, my_row = info_ref[0], info_ref[1]
    upper0 = upper_ref[...].reshape(width, width)
    upper0 = jnp.where(first & (my_col == 0), jnp.zeros_like(upper0), upper0)
    upper1 = band_ref[...].reshape(width, width).astype(F32)
    upper1 = (upper1 - jnp.dot(second_ref[...], upper0, preferred_element_type=F32)).astype(BF16)
    upper1 = jnp.where(first & (my_col < 2), jnp.zeros_like(upper1), upper1)
    here, cols = pl.program_id(0), pl.num_programs(0)

    def both(index):
        rows = [own_ref[pl.ds(index, 1), :], total_ref[pl.ds(index, 1), :]]
        return jnp.concatenate(rows + [jnp.zeros((6, width), F32)], axis=0)

    checks = both(here) - times_rows(both(cols), upper0) - times_rows(both(cols + 1), upper1)
    check_ref[0] = checks[0:1]
    sum_ref[pl.ds(here, 1), :] = checks[1:2]
    for a in range(tile_ref.shape[0]):
        rows = slice(a * width, (a + 1) * width)
        tile = tile_ref[a, 0].astype(F32) - jnp.dot(left0_ref[rows, :], upper0, preferred_element_type=F32)
        tile = tile.astype(BF16).astype(F32)
        tile = tile - jnp.dot(left1_ref[rows, :], upper1, preferred_element_type=F32)
        out_ref[a, 0] = tile.astype(BF16)
    for a in range(tile_ref.shape[0]):
        for pivot, left_ref in enumerate((left0_ref, left1_ref)):
            below = True if a > 0 else my_row > pivot

            @pl.when(first & (my_col == pivot) & below)
            def _():
                out_ref[a, 0] = left_ref[a * width : (a + 1) * width, :]


def eliminate(matrix, multiplier, checksum_weight):
    block_rows, block, cols, _ = matrix.shape
    grid_rows, grid_cols = lax.axis_size(ROW), lax.axis_size("col")
    my_row, my_col = lax.axis_index(ROW), lax.axis_index("col")
    info = jnp.stack([my_col, my_row, lax.axis_index("row_1")]).astype(jnp.int32)
    tiles = matrix.transpose(0, 2, 1, 3)
    rows, piece = block_rows * block, block // grid_rows
    weights = jnp.pad(checksum_weight.reshape(1, rows), ((0, 7), (0, 0)))
    smem = pl.BlockSpec(memory_space=pltpu.SMEM)
    column_of_tiles = pl.BlockSpec((block_rows, 1, block, block), lambda c: (0, c, 0, 0))
    one_check = pl.BlockSpec((1, 8, block), lambda c: (c, 0, 0))

    sides = lax.axis_size("row_1")
    my_y, my_z = lax.axis_index("row_0"), lax.axis_index("row_1")

    bands = pl.pallas_call(
        bands_kernel,
        out_shape=jax.ShapeDtypeStruct((grid_rows, cols, piece, block), BF16),
        grid=(2,),
        in_specs=[pl.BlockSpec((cols // 2, grid_rows, piece, block), lambda c: (c, 0, 0, 0))],
        out_specs=pl.BlockSpec((grid_rows, cols // 2, piece, block), lambda c: (0, c, 0, 0)),
        cost_estimate=pl.CostEstimate(flops=cols * block * block, bytes_accessed=4 * cols * block * block, transcendentals=0),
        name="bands",
    )(tiles.reshape(block_rows * cols, grid_rows, piece, block))
    bands = lax.all_to_all(bands, ROW, 0, 0)
    upper = lax.all_gather(bands[:2], ROW).reshape(grid_rows, 2 * cols, piece, block)

    strip = block // grid_cols
    deep = tiles.reshape(block_rows, cols, grid_cols, strip, block)
    cell = jax.ShapeDtypeStruct((block_rows, strip, block), BF16)
    cells = pl.pallas_call(
        panels_kernel,
        out_shape=(cell,) * grid_cols,
        grid=(1,),
        in_specs=[smem, pl.BlockSpec((block_rows, 1, grid_cols, strip, block), lambda j: (0, 0, 0, 0, 0))],
        out_specs=(pl.BlockSpec((block_rows, strip, block), lambda j: (0, 0, 0)),) * grid_cols,
        cost_estimate=pl.CostEstimate(flops=rows * block, bytes_accessed=4 * rows * block, transcendentals=0),
        name="panels",
    )(info, deep)
    panels = shifts("col", cells, lambda s: [(0, s), (1, (1 + s) % grid_cols)])
    panel0, panel1 = from_two(panels, my_col)
    panels = jnp.stack([panel0, panel1])
    around = lambda s: [(i, (i + s) % grid_cols) for i in range(grid_cols)]
    panels = shifts("col", [panels] * grid_cols, around)

    corner = jnp.where(my_row == 1, panel0[0], panel1[0])
    corner = shifts("row_1", [corner] * sides, lambda s: [(0, s), (1, (1 + s) % sides)])
    corner = jnp.stack(from_two(corner, my_z))
    corner = shifts("row_0", [corner] * sides, lambda s: [(0, s)])
    corner = lax.select_n(my_y, *corner)
    around = lambda s: [(i, (i + s) % grid_cols) for i in range(grid_cols)]
    corner = shifts("col", [corner] * grid_cols, around)
    ordered = corner[::-1]
    ordered = lax.dynamic_slice_in_dim(jnp.stack(ordered + ordered[:-1]), grid_cols - 1 - my_col, grid_cols, 0)
    corners = ordered.transpose(1, 0, 2, 3).reshape(2, block, block)

    base = pl.pallas_call(
        weigh_kernel,
        out_shape=jax.ShapeDtypeStruct((cols, 8, block), F32),
        grid=(cols,),
        in_specs=[pl.BlockSpec((8, rows), lambda c: (0, 0)), column_of_tiles],
        out_specs=one_check,
        cost_estimate=pl.CostEstimate(flops=64 * tiles.size, bytes_accessed=2 * tiles.size, transcendentals=0),
        name="weigh",
    )(weights, tiles)

    left0, left1, sums = pl.pallas_call(
        functools.partial(left_kernel, grid_cols),
        out_shape=(
            jax.ShapeDtypeStruct((rows, block), BF16),
            jax.ShapeDtypeStruct((rows, block), BF16),
            jax.ShapeDtypeStruct((2, 8, block), F32),
        ),
        in_specs=[smem] + [pl.BlockSpec(memory_space=pltpu.VMEM)] * (3 + grid_cols),
        out_specs=(pl.BlockSpec(memory_space=pltpu.VMEM),) * 3,
        cost_estimate=pl.CostEstimate(flops=6 * rows * block * block, bytes_accessed=12 * rows * block, transcendentals=0),
        compiler_params=pltpu.CompilerParams(vmem_limit_bytes=24 << 20),
        name="left",
    )(info, corners[0], multiplier, weights, *panels)
    second_left = jnp.dot(corners[1], multiplier[0], preferred_element_type=F32).astype(BF16)

    own = jnp.concatenate([base[:, 0], sums[:, 0]], axis=0)
    total = own
    for axis in ("row_1", "row_0"):
        around = lambda s: [(i, (i + s) % sides) for i in range(sides)]
        total = functools.reduce(jnp.add, shifts(axis, [total] * sides, around))

    whole = lambda *shape: pl.BlockSpec(shape, lambda c: (0,) * len(shape))
    out, checks, totals = pl.pallas_call(
        trail_kernel,
        out_shape=(
            jax.ShapeDtypeStruct(tiles.shape, BF16),
            jax.ShapeDtypeStruct((cols, 1, block), F32),
            jax.ShapeDtypeStruct((cols, block), F32),
        ),
        grid=(cols,),
        in_specs=[
            smem,
            whole(rows, block),
            whole(rows, block),
            whole(block, block),
            whole(cols + 2, block),
            whole(cols + 2, block),
            pl.BlockSpec((grid_rows, 1, piece, block), lambda c: (0, c, 0, 0)),
            pl.BlockSpec((grid_rows, 1, piece, block), lambda c: (0, c + cols, 0, 0)),
            column_of_tiles,
        ],
        out_specs=(column_of_tiles, pl.BlockSpec((1, 1, block), lambda c: (c, 0, 0)), whole(cols, block)),
        cost_estimate=pl.CostEstimate(flops=5 * rows * block * block * cols, bytes_accessed=4 * tiles.size, transcendentals=0),
        name="trail",
    )(info, left0, left1, second_left, own, total, upper, upper, tiles)
    return out.transpose(0, 2, 1, 3), checks.transpose(1, 0, 2), totals


def solution(mesh):
    split = Mesh(mesh.devices.reshape(4, 4, mesh.shape["col"]), ("row_0", "row_1", "col"))
    in_specs = (P(None, ROW, None, "col"), P(), P(None, ROW))
    out_specs = (P(None, ROW, None, "col"), P(ROW, None, "col"), P(None, "col"))
    return jax.shard_map(eliminate, mesh=split, in_specs=in_specs, out_specs=out_specs, check_vma=False)
```

```python
import functools

import jax
import jax.numpy as jnp
from jax import lax
from jax.experimental import pallas as pl
from jax.experimental.pallas import tpu as pltpu
from jax.sharding import Mesh
from jax.sharding import PartitionSpec as P

ROW = ("row_0", "row_1")
F32, BF16 = jnp.float32, jnp.bfloat16


def shifts(axis, pieces, pairs):
    return [pieces[0]] + [lax.ppermute(p, axis, pairs(s)) for s, p in enumerate(pieces) if s > 0]


def from_two(got, place):
    size = len(got)
    return lax.select_n(place, *got), lax.select_n((place + size - 1) % size, *got)


def bands_kernel(tile_ref, out_ref):
    for c in range(tile_ref.shape[0]):
        out_ref[:, c] = tile_ref[c]


def panels_kernel(info_ref, panel_ref, *out_refs):
    parts = len(out_refs)
    for s in range(parts):
        out_refs[s][...] = panel_ref[:, 0, lax.rem(info_ref[0] + s, parts)]


def in_three(rows):
    high = rows.astype(BF16).astype(F32)
    middle = (rows - high).astype(BF16).astype(F32)
    low = rows - high - middle
    return jnp.concatenate([high, middle, low, jnp.zeros_like(rows)], axis=0).astype(BF16)


def times_rows(rows, right):
    product = jnp.dot(in_three(rows), right, preferred_element_type=F32)
    return product[0:8] + product[8:16] + product[16:24]


def weigh_kernel(weight_ref, tile_ref, out_ref):
    block_rows, _, width, _ = tile_ref.shape
    tile = tile_ref[...].reshape(block_rows * width, width)
    out_ref[0] = times_rows(weight_ref[...], tile)


def left_kernel(strips, info_ref, corner_ref, multiplier_ref, weight_ref, *refs):
    panel_refs, (left0_ref, left1_ref, sum_ref) = refs[:strips], refs[strips:]
    width = corner_ref.shape[0]
    _, block_rows, strip, _ = panel_refs[0].shape
    row = lax.broadcasted_iota(jnp.int32, (block_rows * width, width), 0)

    def column(step):
        parts = [ref[step, a] for a in range(block_rows) for ref in panel_refs]
        return jnp.concatenate(parts, axis=0)

    def finish(step, factor, left_ref):
        left = jnp.dot(factor, multiplier_ref[step], preferred_element_type=F32)
        left = jnp.where((row < width) & (info_ref[1] <= step), jnp.zeros_like(left), left).astype(BF16)
        for s in range(strips):
            place = lax.rem(info_ref[0] - s + strips, strips) * strip
            for a in range(block_rows):
                at = pl.multiple_of(a * width + place, strip)
                start = (a * strips + s) * strip
                left_ref[pl.ds(at, strip), :] = left[start : start + strip]
        sum_ref[step] = times_rows(weight_ref[...], left_ref[...])
        return left

    left0 = finish(0, column(0), left0_ref)
    update = jnp.dot(left0, corner_ref[...], preferred_element_type=F32)
    finish(1, (column(1).astype(F32) - update).astype(BF16), left1_ref)


def trail_kernel(
    info_ref, left0_ref, left1_ref, second_ref, own_ref, total_ref, upper_ref, band_ref, tile_ref,
    out_ref, check_ref, sum_ref, longer0_ref, longer1_ref
):
    width = second_ref.shape[0]
    first = pl.program_id(0) == 0
    my_col, my_row = info_ref[0], info_ref[1]
    here, cols, last = pl.program_id(0), pl.num_programs(0), tile_ref.shape[0] - 1

    def both(index):
        rows = [own_ref[pl.ds(index, 1), :], total_ref[pl.ds(index, 1), :]]
        return jnp.concatenate(rows + [jnp.zeros((6, width), F32)], axis=0)

    @pl.when(first)
    def _():
        longer0_ref[:width] = second_ref[...]
        longer0_ref[width:] = in_three(both(cols))
        longer1_ref[:width] = left1_ref[last * width :, :]
        longer1_ref[width:] = in_three(both(cols + 1))

    def split(product):
        rows = product[width:]
        return product[:width], rows[0:8] + rows[8:16] + rows[16:24]

    upper0 = upper_ref[...].reshape(width, width)
    upper0 = jnp.where(first & (my_col == 0), jnp.zeros_like(upper0), upper0)
    product, checks0 = split(jnp.dot(longer0_ref[...], upper0, preferred_element_type=F32))
    upper1 = (band_ref[...].reshape(width, width).astype(F32) - product).astype(BF16)
    upper1 = jnp.where(first & (my_col < 2), jnp.zeros_like(upper1), upper1)
    for a in range(last + 1):
        rows = slice(a * width, (a + 1) * width)
        tile = tile_ref[a, 0].astype(F32) - jnp.dot(left0_ref[rows, :], upper0, preferred_element_type=F32)
        tile = tile.astype(BF16).astype(F32)
        if a < last:
            product = jnp.dot(left1_ref[rows, :], upper1, preferred_element_type=F32)
        else:
            product, checks1 = split(jnp.dot(longer1_ref[...], upper1, preferred_element_type=F32))
        out_ref[a, 0] = (tile - product).astype(BF16)
    checks = both(here) - checks0 - checks1
    check_ref[0] = checks[0:1]
    sum_ref[pl.ds(here, 1), :] = checks[1:2]
    for a in range(tile_ref.shape[0]):
        for pivot, left_ref in enumerate((left0_ref, left1_ref)):
            below = True if a > 0 else my_row > pivot

            @pl.when(first & (my_col == pivot) & below)
            def _():
                out_ref[a, 0] = left_ref[a * width : (a + 1) * width, :]


def eliminate(matrix, multiplier, checksum_weight):
    block_rows, block, cols, _ = matrix.shape
    grid_rows, grid_cols = lax.axis_size(ROW), lax.axis_size("col")
    my_row, my_col = lax.axis_index(ROW), lax.axis_index("col")
    info = jnp.stack([my_col, my_row, lax.axis_index("row_1")]).astype(jnp.int32)
    tiles = matrix.transpose(0, 2, 1, 3)
    rows, piece = block_rows * block, block // grid_rows
    weights = jnp.pad(checksum_weight.reshape(1, rows), ((0, 7), (0, 0)))
    smem = pl.BlockSpec(memory_space=pltpu.SMEM)
    column_of_tiles = pl.BlockSpec((block_rows, 1, block, block), lambda c: (0, c, 0, 0))
    one_check = pl.BlockSpec((1, 8, block), lambda c: (c, 0, 0))

    sides = lax.axis_size("row_1")
    my_y, my_z = lax.axis_index("row_0"), lax.axis_index("row_1")

    bands = pl.pallas_call(
        bands_kernel,
        out_shape=jax.ShapeDtypeStruct((grid_rows, cols, piece, block), BF16),
        grid=(2,),
        in_specs=[pl.BlockSpec((cols // 2, grid_rows, piece, block), lambda c: (c, 0, 0, 0))],
        out_specs=pl.BlockSpec((grid_rows, cols // 2, piece, block), lambda c: (0, c, 0, 0)),
        cost_estimate=pl.CostEstimate(flops=cols * block * block, bytes_accessed=4 * cols * block * block, transcendentals=0),
        name="bands",
    )(tiles.reshape(block_rows * cols, grid_rows, piece, block))
    bands = lax.all_to_all(bands, ROW, 0, 0)
    upper = lax.all_gather(bands[:2], ROW).reshape(grid_rows, 2 * cols, piece, block)

    strip = block // grid_cols
    deep = tiles.reshape(block_rows, cols, grid_cols, strip, block)
    cell = jax.ShapeDtypeStruct((block_rows, strip, block), BF16)
    cells = pl.pallas_call(
        panels_kernel,
        out_shape=(cell,) * grid_cols,
        grid=(1,),
        in_specs=[smem, pl.BlockSpec((block_rows, 1, grid_cols, strip, block), lambda j: (0, 0, 0, 0, 0))],
        out_specs=(pl.BlockSpec((block_rows, strip, block), lambda j: (0, 0, 0)),) * grid_cols,
        cost_estimate=pl.CostEstimate(flops=rows * block, bytes_accessed=4 * rows * block, transcendentals=0),
        name="panels",
    )(info, deep)
    panels = shifts("col", cells, lambda s: [(0, s), (1, (1 + s) % grid_cols)])
    panel0, panel1 = from_two(panels, my_col)
    panels = jnp.stack([panel0, panel1])
    around = lambda s: [(i, (i + s) % grid_cols) for i in range(grid_cols)]
    panels = shifts("col", [panels] * grid_cols, around)

    corner = jnp.where(my_row == 1, panel0[0], panel1[0])
    corner = shifts("row_1", [corner] * sides, lambda s: [(0, s), (1, (1 + s) % sides)])
    corner = jnp.stack(from_two(corner, my_z))
    corner = shifts("row_0", [corner] * sides, lambda s: [(0, s)])
    corner = lax.select_n(my_y, *corner)
    around = lambda s: [(i, (i + s) % grid_cols) for i in range(grid_cols)]
    corner = shifts("col", [corner] * grid_cols, around)
    ordered = corner[::-1]
    ordered = lax.dynamic_slice_in_dim(jnp.stack(ordered + ordered[:-1]), grid_cols - 1 - my_col, grid_cols, 0)
    corners = ordered.transpose(1, 0, 2, 3).reshape(2, block, block)

    base = pl.pallas_call(
        weigh_kernel,
        out_shape=jax.ShapeDtypeStruct((cols, 8, block), F32),
        grid=(cols,),
        in_specs=[pl.BlockSpec((8, rows), lambda c: (0, 0)), column_of_tiles],
        out_specs=one_check,
        cost_estimate=pl.CostEstimate(flops=64 * tiles.size, bytes_accessed=2 * tiles.size, transcendentals=0),
        name="weigh",
    )(weights, tiles)

    left0, left1, sums = pl.pallas_call(
        functools.partial(left_kernel, grid_cols),
        out_shape=(
            jax.ShapeDtypeStruct((rows, block), BF16),
            jax.ShapeDtypeStruct((rows, block), BF16),
            jax.ShapeDtypeStruct((2, 8, block), F32),
        ),
        in_specs=[smem] + [pl.BlockSpec(memory_space=pltpu.VMEM)] * (3 + grid_cols),
        out_specs=(pl.BlockSpec(memory_space=pltpu.VMEM),) * 3,
        cost_estimate=pl.CostEstimate(flops=6 * rows * block * block, bytes_accessed=12 * rows * block, transcendentals=0),
        compiler_params=pltpu.CompilerParams(vmem_limit_bytes=24 << 20),
        name="left",
    )(info, corners[0], multiplier, weights, *panels)
    second_left = jnp.dot(corners[1], multiplier[0], preferred_element_type=F32).astype(BF16)

    own = jnp.concatenate([base[:, 0], sums[:, 0]], axis=0)
    total = own
    for axis in ("row_1", "row_0"):
        around = lambda s: [(i, (i + s) % sides) for i in range(sides)]
        total = functools.reduce(jnp.add, shifts(axis, [total] * sides, around))

    whole = lambda *shape: pl.BlockSpec(shape, lambda c: (0,) * len(shape))
    out, checks, totals = pl.pallas_call(
        trail_kernel,
        out_shape=(
            jax.ShapeDtypeStruct(tiles.shape, BF16),
            jax.ShapeDtypeStruct((cols, 1, block), F32),
            jax.ShapeDtypeStruct((cols, block), F32),
        ),
        grid=(cols,),
        in_specs=[
            smem,
            whole(rows, block),
            whole(rows, block),
            whole(block, block),
            whole(cols + 2, block),
            whole(cols + 2, block),
            pl.BlockSpec((grid_rows, 1, piece, block), lambda c: (0, c, 0, 0)),
            pl.BlockSpec((grid_rows, 1, piece, block), lambda c: (0, c + cols, 0, 0)),
            column_of_tiles,
        ],
        out_specs=(column_of_tiles, pl.BlockSpec((1, 1, block), lambda c: (c, 0, 0)), whole(cols, block)),
        scratch_shapes=[pltpu.VMEM((block + 32, block), BF16)] * 2,
        cost_estimate=pl.CostEstimate(flops=5 * rows * block * block * cols, bytes_accessed=4 * tiles.size, transcendentals=0),
        name="trail",
    )(info, left0, left1, second_left, own, total, upper, upper, tiles)
    return out.transpose(0, 2, 1, 3), checks.transpose(1, 0, 2), totals


def solution(mesh):
    split = Mesh(mesh.devices.reshape(4, 4, mesh.shape["col"]), ("row_0", "row_1", "col"))
    in_specs = (P(None, ROW, None, "col"), P(), P(None, ROW))
    out_specs = (P(None, ROW, None, "col"), P(ROW, None, "col"), P(None, "col"))
    return jax.shard_map(eliminate, mesh=split, in_specs=in_specs, out_specs=out_specs, check_vma=False)
```
